32 devices in a mesh: dp: 4 (over x, core), mp: 8 (over z, y).
Axes of the slice: x: 2, y: 2, z: 4, core: 2. Of those that a mesh axis runs over, the one named last changes fastest.
Arguments:
- tokens: bfloat16 [1024, 8192], P('dp'), may hold values from -6 to 6
- norm_gain: float32 [8192], replicated, may hold values from 0.5 to 1.5
- gate_weight: bfloat16 [8192, 28672], P('dp', 'mp'), may hold values from -0.0625 to 0.0625
- gate_mask: int32 [8192, 896], P('dp', 'mp'), may hold values from -2147483648 to 2147483646
- up_weight: bfloat16 [8192, 28672], P('dp', 'mp'), may hold values from -0.0625 to 0.0625
- up_mask: int32 [8192, 896], P('dp', 'mp'), may hold values from -2147483648 to 2147483646
- down_weight: bfloat16 [28672, 8192], P('mp', 'dp'), may hold values from -0.03125 to 0.03125
- down_mask: int32 [28672, 256], P('mp', 'dp'), may hold values from -2147483648 to 2147483647, as said below
Outputs:
- mixed: bfloat16 [1024, 8192], P('mp', 'dp')
- input_norms: float32 [8192], P('dp')
- hidden_norms: float32 [28672], P('mp')
The draws below stay inside these ranges and needn't reach their ends.
Inputs may be any that keep to these rules, and one draw needn't show every extreme that they name: `down_mask`: in every word each of the eight aligned groups of four bits holds exactly two ones, so exactly two of every four consecutive columns of the down projection are kept.
All inputs are finite; a program needn't handle non-finite values.
Results may differ from the reference program's by a relative error of at most 0.025.
Values may be sent and summed in bfloat16 or wider, within the bound.
A program may use at most 192 MiB of HBM per device.

```python
import jax
import jax.numpy as jnp
from jax import lax

D = 8192
FF = 28672
TOKENS = 1024
N_DP = 4
N_MP = 8


def draw_down_mask(key, part):
    patterns = jnp.array([3, 5, 6, 9, 10, 12], jnp.int32)
    selected = jax.random.randint(key, (FF, D // 32, 8), 0, 6, dtype=jnp.int32)
    nibbles = patterns[selected]
    shifts = 4 * jnp.arange(8, dtype=jnp.int32)
    placed = jnp.left_shift(nibbles, shifts)
    return jnp.sum(placed, axis=2, dtype=jnp.int32)


def set_ends(entries, rng, least, largest):
    longest = entries.shape.index(max(entries.shape))
    spots = []
    for shift in (0, 1):
        where = [jax.random.randint(jax.random.fold_in(rng, axis), (), 0, length) for axis, length in enumerate(entries.shape)]
        where[longest] = (where[longest] + shift) % entries.shape[longest]
        spots.append(tuple(where))
    return entries.at[spots[0]].set(least).at[spots[1]].set(largest)


def level_of(key, shape, split, smallest, high):
    def one(axis_at, blocks):
        heights = jax.random.uniform(jax.random.fold_in(jax.random.fold_in(key, 6), axis_at), (blocks,), jnp.float32, smallest / len(split), high / len(split))
        return jnp.repeat(jnp.exp(heights), shape[axis_at] // blocks).reshape((-1,) + (1,) * (len(shape) - axis_at - 1))

    level = one(*split[0])
    for cut in split[1:]:
        level = level * one(*cut)
    return level


def centred(stream_key, extent, width, most, cuts=(), kind=jnp.bfloat16):
    gain = level_of(stream_key, extent, cuts, -0.22, 0.18) if cuts else 1.0
    entries = jax.random.normal(stream_key, extent, jnp.float32) * width * gain
    return jnp.minimum(jnp.maximum(entries, -most), most).astype(kind)


def setup_inputs(seed: int = 0) -> dict:
    keys = jax.random.split(jax.random.key(seed), 9)
    tokens = centred(keys[0], (TOKENS, D), 1.0, 6.0, ((0, 4),))
    norm_gain = jnp.clip(1.0 + 0.1 * jax.random.normal(keys[1], (D,), jnp.float32), 0.5, 1.5)
    gate_weight = centred(keys[2], (D, FF), D ** -0.5, 0.0625, ((0, 4), (1, 8)))
    gate_mask = set_ends(jax.random.randint(keys[3], (D, FF // 32), -2147483648, 2147483647), jax.random.fold_in(keys[3], 1), -2147483648, 2147483646).astype(jnp.int32)
    up_weight = centred(keys[4], (D, FF), D ** -0.5, 0.0625, ((0, 4), (1, 8)))
    up_mask = set_ends(jax.random.randint(keys[5], (D, FF // 32), -2147483648, 2147483647), jax.random.fold_in(keys[5], 1), -2147483648, 2147483646).astype(jnp.int32)
    down_weight = centred(keys[6], (FF, D), FF ** -0.5, 0.03125, ((0, 8), (1, 4)))
    down_mask = draw_down_mask(jax.random.fold_in(keys[8], 71), 0)
    return dict(tokens=tokens, norm_gain=norm_gain, gate_weight=gate_weight, gate_mask=gate_mask, up_weight=up_weight, up_mask=up_mask, down_weight=down_weight, down_mask=down_mask)


def keep_entries(weight, packed):
    shifts = jnp.arange(32, dtype=jnp.int32)
    kept_bits = jnp.right_shift(packed[..., None], shifts) & 1
    kept_bits = kept_bits.reshape(weight.shape)
    return jnp.where(kept_bits == 1, weight, jnp.zeros_like(weight))

def reference(tokens, norm_gain, gate_weight, gate_mask, up_weight, up_mask, down_weight, down_mask):
    values = tokens.astype(jnp.float32)
    scale = lax.rsqrt(lax.optimization_barrier(jnp.mean(values * values, axis=1, keepdims=True)) + 1e-05)
    normed = (values * scale * norm_gain).astype(jnp.bfloat16)
    widened = normed.astype(jnp.float32)
    input_norms = jnp.sqrt(lax.optimization_barrier(jnp.sum(widened * widened, axis=0)))
    stride = D // N_DP

    def add_block(position, sums_so_far):
        gate_sum, up_sum = sums_so_far
        offset = (position * stride).astype(jnp.int32)
        row_block = lax.dynamic_slice_in_dim(normed, offset, stride, 1)
        gate_rows = keep_entries(lax.dynamic_slice_in_dim(gate_weight, offset, stride, 0), lax.dynamic_slice_in_dim(gate_mask, offset, stride, 0))
        up_rows = keep_entries(lax.dynamic_slice_in_dim(up_weight, offset, stride, 0), lax.dynamic_slice_in_dim(up_mask, offset, stride, 0))
        gate_part = jnp.dot(row_block, gate_rows, preferred_element_type=jnp.float32).astype(jnp.bfloat16)
        up_part = jnp.dot(row_block, up_rows, preferred_element_type=jnp.float32).astype(jnp.bfloat16)
        gate_part, up_part = lax.optimization_barrier((gate_part, up_part))
        return (gate_sum + gate_part.astype(jnp.float32), up_sum + up_part.astype(jnp.float32))
    zeros_sum = jnp.zeros((normed.shape[0], FF), jnp.float32)
    gate, up = lax.fori_loop(0, N_DP, add_block, (zeros_sum, zeros_sum))
    hidden = (jax.nn.silu(gate) * up).astype(jnp.bfloat16)
    wide_hidden = hidden.astype(jnp.float32)
    hidden_norms = jnp.sqrt(lax.optimization_barrier(jnp.sum(wide_hidden * wide_hidden, axis=0)))
    unit_stride = FF // N_MP

    def add_down(position, running):
        offset = (position * unit_stride).astype(jnp.int32)
        row_block = lax.dynamic_slice_in_dim(hidden, offset, unit_stride, 1)
        down_rows = keep_entries(lax.dynamic_slice_in_dim(down_weight, offset, unit_stride, 0), lax.dynamic_slice_in_dim(down_mask, offset, unit_stride, 0))
        return running + jnp.dot(row_block, down_rows, preferred_element_type=jnp.float32)
    mixed = lax.fori_loop(0, N_MP, add_down, jnp.zeros((normed.shape[0], D), jnp.float32))
    return (mixed.astype(jnp.bfloat16), input_norms, hidden_norms)
```

```python
import functools

import jax
import jax.numpy as jnp
from jax import lax
from jax.experimental import pallas as pl
from jax.experimental.pallas import tpu as pltpu
from jax.sharding import PartitionSpec as P

CORES = 2
CHUNKS = 4
GROUPS = ((0, 1), (2,), (3,))
TILE = 256
PIECE = 512
SLOTS = 4
MESH = pl.DeviceIdType.MESH
BF16 = jnp.bfloat16
F32 = jnp.float32


def norm_kernel(tokens_ref, gain_ref, normed_ref):
    values = tokens_ref[...].astype(F32)
    scale = lax.rsqrt(jnp.mean(values * values, axis=1, keepdims=True) + 1e-05)
    normed_ref[...] = (values * scale * gain_ref[...]).astype(BF16)


def normalise(tokens, norm_gain):
    rows, features = tokens.shape
    block = 32
    return pl.pallas_call(
        norm_kernel,
        grid=(rows // block,),
        in_specs=[
            pl.BlockSpec((block, features), lambda i: (i, 0)),
            pl.BlockSpec((1, features), lambda i: (0, 0)),
        ],
        out_specs=pl.BlockSpec((block, features), lambda i: (i, 0)),
        out_shape=jax.ShapeDtypeStruct(tokens.shape, BF16),
        cost_estimate=pl.CostEstimate(
            flops=5 * rows * features, bytes_accessed=4 * rows * features, transcendentals=rows
        ),
    )(tokens, norm_gain[None, :])


def keep_tile(words_ref, word, row):
    block = words_ref[pl.ds(pl.multiple_of(word, 8), 8), pl.ds(pl.multiple_of(row, 128), 128)]
    spread = jnp.concatenate([jnp.broadcast_to(block[w : w + 1], (32, 128)) for w in range(8)], axis=0)
    shifts = 31 - lax.broadcasted_iota(jnp.int32, (TILE, 128), 0) % 32
    kept = jnp.left_shift(spread, shifts) < 0
    return jnp.where(kept, 1.0, 0.0).astype(BF16).T


def layer_kernel(
    n_dp, n_mp, levels,
    normed, gate_weight, up_weight, down_weight, gate_words, up_words, down_words,
    mixed, input_norms, hidden_norms, kept_down,
    xs, kept, raw, words, dwords, pair_out, pair_in, mine, sent, arrived, hs, po, land,
    load_sem, raw_sem, tile_sem, xp_sem, xx_sem, rd_sem, pair_sem, p_sem, h_sem, hp_sem, e_sem,
):
    chips = n_dp // CORES
    width, units = gate_weight.shape
    blocks = units // TILE
    tiles = width // TILE
    pieces = width // PIECE
    piece_rows = xs.shape[-2]
    rows = piece_rows * n_mp
    shards = n_mp // n_dp
    small = rows // CHUNKS
    part = small // shards
    p, m = lax.axis_index("dp"), lax.axis_index("mp")
    chip, core = p // CORES, p % CORES
    partner = chip * CORES + (1 - core)
    bits = [m // 2**level % 2 for level in range(levels)]
    every = slice(None)

    def chip_at(shift):
        return lax.rem(chip + (shift % chips), chips)

    def device(which_chip, which_core):
        return which_chip * CORES + which_core

    def across(level):
        return m + (1 - 2 * bits[level]) * 2**level

    def remote(source, target, sems, index, to_dp, to_mp):
        return pltpu.make_async_remote_copy(
            src_ref=source,
            dst_ref=target,
            send_sem=sems.at[(0,) + index],
            recv_sem=sems.at[(1,) + index],
            device_id=(to_dp, to_mp),
            device_id_type=MESH,
        )

    barrier = pltpu.get_barrier_semaphore()
    peers = [(partner, m)]
    for shift in range(1, chips):
        peers += [(device(chip_at(shift), which), m) for which in range(CORES)]
    peers += [(p, across(level)) for level in range(levels)]
    for to_dp, to_mp in peers:
        pl.semaphore_signal(barrier, inc=1, device_id=(to_dp, to_mp), device_id_type=MESH)

    loads = [
        pltpu.make_async_copy(gate_words, words.at[0], load_sem.at[0]),
        pltpu.make_async_copy(up_words, words.at[1], load_sem.at[1]),
        pltpu.make_async_copy(down_words, dwords, load_sem.at[2]),
    ]
    own_features = (every,) * (levels + 1) + (pl.ds(pl.multiple_of(p * width, width), width),)
    own_load = pltpu.make_async_copy(normed.at[own_features], xs.at[p], load_sem.at[3])
    own_load.start()
    loads[0].start()
    loads[1].start()

    def raw_loads(block, slot):
        span = pl.ds(pl.multiple_of(block * TILE, TILE), TILE)
        return [
            pltpu.make_async_copy(
                weight.at[:, span], raw.at[slot, pl.ds(which * width, width)], raw_sem.at[slot, which]
            )
            for which, weight in enumerate((gate_weight, up_weight))
        ]

    for copy in raw_loads(0, 0):
        copy.start()
    loads[2].start()
    pl.semaphore_wait(barrier, len(peers))

    def features_of(where):
        return pl.ds(pl.multiple_of(where * width, width), width)

    to_partner = remote(
        normed.at[(every,) * (levels + 1) + (features_of(partner),)], xs.at[p], xp_sem, (), partner, m
    )
    from_partner = remote(
        normed.at[(every,) * (levels + 1) + (features_of(partner),)], xs.at[partner], xp_sem, (), partner, m
    )
    to_partner.start()
    my_piece = tuple(bits[level] for level in reversed(range(levels)))
    shared = []
    for shift in range(1, chips):
        for which in range(CORES):
            target = device(chip_at(shift), which)
            shared.append(
                remote(
                    normed.at[my_piece + (every, features_of(target))],
                    xs.at[(p,) + my_piece],
                    xx_sem, (shift - 1, which, core), target, m,
                )
            )
            shared[-1].start()

    def spread_copies(step):
        level = levels - 1 - step
        fixed = tuple(bits[low] for low in reversed(range(level + 1)))
        copies = []
        for shift in range(1, chips):
            for which in range(CORES):
                source = device(chip_at(-shift), which)
                view = xs.at[(source,) + (every,) * step + fixed]
                copies.append(remote(view, view, rd_sem, (step, shift - 1, which), p, across(level)))
        return copies

    def spread_waits(step):
        level = levels - 1 - step
        fixed = (1 - bits[level],) + tuple(bits[low] for low in reversed(range(level)))
        for shift in range(1, chips):
            for which in range(CORES):
                source = device(chip_at(-shift), which)
                view = xs.at[(source,) + (every,) * step + fixed]
                remote(view, view, rd_sem, (step, shift - 1, which), p, across(level)).wait_recv()

    def spread_step(step):
        if step == 0:
            for shift in range(1, chips):
                for which in range(CORES):
                    source = device(chip_at(-shift), which)
                    view = xs.at[(source,) + my_piece]
                    remote(view, view, xx_sem, (shift - 1, core, which), p, m).wait_recv()
        else:
            spread_waits(step - 1)
        for copy in spread_copies(step):
            copy.start()

    def finish_spread():
        if chips > 1:
            spread_waits(levels - 1)
            for step in range(levels):
                for copy in spread_copies(step):
                    copy.wait_send()
            for copy in shared:
                copy.wait_send()

    def piece_index(piece):
        return tuple(piece // 2**level % 2 for level in reversed(range(levels)))

    def token_rows(source, group):
        values = []
        for chunk in group:
            for shard in range(shards):
                first = (shard * rows // shards + chunk * part) // piece_rows
                for piece in range(first, first + part // piece_rows):
                    values.append(xs[(source,) + piece_index(piece)])
        return values

    clock = [0]

    def pair_copy(turn, count):
        slot = turn % SLOTS
        return remote(
            pair_out.at[slot, pl.ds(0, count)], pair_in.at[slot, pl.ds(0, count)], pair_sem, (slot,), partner, m
        )

    def partials(group, shift, prepare, finish):
        count = small * len(group)
        which = chip_at(shift)
        base = clock[0]
        clock[0] = base + blocks

        def settle(block):
            turn = base + block
            copy = pair_copy(turn, count)
            copy.wait()
            slot = turn % SLOTS
            finish(block, mine[turn % 2, pl.ds(0, count)] + pair_in[slot, pl.ds(0, count)].astype(F32))

        def step(block, carry):
            turn = base + block
            prepare(block)
            left = jnp.concatenate(
                token_rows(device(which, core), group) + token_rows(device(which, 1 - core), group), axis=0
            )
            product = jnp.dot(left, kept[block], preferred_element_type=F32)
            pair_out[turn % SLOTS, pl.ds(0, count)] = product[count:].astype(BF16)
            pair_copy(turn, count).start()
            mine[turn % 2, pl.ds(0, count)] = product[:count].astype(BF16).astype(F32)

            @pl.when(block > 0)
            def _():
                settle(block - 1)

            return carry

        lax.fori_loop(0, blocks, step, 0)
        settle(blocks - 1)

    def mask_block(block):
        slot = block % 2
        for copy in raw_loads(block, slot):
            copy.wait()

        @pl.when(block + 1 < blocks)
        def _():
            for copy in raw_loads(block + 1, 1 - slot):
                copy.start()

        def band(index, carry):
            for inner in range(2):
                row = pl.multiple_of(index * TILE + inner * 128, 128)
                for which in range(2):
                    ones = keep_tile(words.at[which], block * 8, row)
                    values = raw[slot, pl.ds(pl.multiple_of(which * width + row, 128), 128)]
                    kept[block, pl.ds(row, 128), which * TILE : which * TILE + TILE] = values * ones
            return carry

        lax.fori_loop(0, width // TILE, band, 0)

    def spread_at(step):
        return max((step + 1) * blocks // (levels + 1) - 1, 0)

    def first_prepare(block):
        mask_block(block)
        if chips > 1:
            for step in range(levels):

                @pl.when(block == spread_at(step))
                def _(step=step):
                    spread_step(step)

    def nothing(block):
        pass

    def sum_copy(number, shift, block, to_chip):
        count = small * len(GROUPS[number])
        return remote(
            sent[number].at[shift, block],
            arrived[number].at[shift, block],
            p_sem, (number, shift, block), device(to_chip, core), m,
        )

    def send_sums(number, shift):
        def finish(block, total):
            sent[number][shift, block] = total.astype(BF16)
            sum_copy(number, shift, block, chip_at(shift + 1)).start()

        return finish

    def away(number, shift, prepare=nothing):
        partials(GROUPS[number], shift, prepare, send_sums(number, shift))

    def hold_source(shift, which_core):
        return device(chip_at(-shift - 1), which_core)

    def make_hidden(number):
        group = GROUPS[number]

        def finish(block, total):
            gate, up = total[:, :TILE], total[:, TILE:]
            for shift in range(chips - 1):
                sum_copy(number, shift, block, chip_at(shift + 1)).wait_recv()
                other = arrived[number][shift, block].astype(F32)
                gate = gate + other[:, :TILE]
                up = up + other[:, TILE:]
            hidden = (gate / (1.0 + jnp.exp(-gate)) * up).astype(BF16)
            span = pl.ds(pl.multiple_of(block * TILE, TILE), TILE)
            for place, chunk in enumerate(group):
                hs[chunk, hold_source(0, core), :, span] = hidden[place * small : (place + 1) * small]

        partials(group, chips - 1, nothing, finish)
        for chunk in group:
            for shift in range(1, chips):
                hidden_copy(chunk, shift).start()
            partner_copy(chunk, 0, core).start()

    def hidden_copy(chunk, shift):
        view = hs.at[chunk, hold_source(0, core)]
        return remote(view, view, h_sem, (chunk, shift - 1), device(chip_at(shift), core), m)

    def hidden_arrival(chunk, shift):
        view = hs.at[chunk, hold_source(shift, core)]
        return remote(view, view, h_sem, (chunk, shift - 1), device(chip_at(shift), core), m)

    def partner_copy(chunk, shift, which_core):
        view = hs.at[chunk, hold_source(shift, which_core)]
        return remote(view, view, hp_sem, (chunk, shift), partner, m)

    def gather_hidden(number):
        for chunk in GROUPS[number]:
            for shift in range(1, chips):
                hidden_arrival(chunk, shift).wait_recv()
                partner_copy(chunk, shift, core).start()
        for chunk in GROUPS[number]:
            for shift in range(chips):
                partner_copy(chunk, shift, 1 - core).wait_recv()

    def tile_load(tile, slot):
        return pltpu.make_async_copy(kept_down.at[tile], raw.at[slot, pl.ds(0, units)], tile_sem.at[0, slot])

    def tile_store(tile, slot):
        return pltpu.make_async_copy(raw.at[slot, pl.ds(0, units)], kept_down.at[tile], tile_sem.at[1, slot])

    def weight_load(tile, slot):
        span = pl.ds(pl.multiple_of(tile * TILE, TILE), TILE)
        return pltpu.make_async_copy(down_weight.at[:, span], raw.at[slot, pl.ds(0, units)], tile_sem.at[0, slot])

    def mask_down():
        weight_load(0, 0).start()

        def step(tile, carry):
            slot = tile % 2
            weight_load(tile, slot).wait()

            @pl.when(tile > 0)
            def _():
                tile_store(tile - 1, 1 - slot).wait()

            @pl.when(tile + 1 < tiles)
            def _():
                weight_load(tile + 1, 1 - slot).start()

            def band(index, carry):
                for inner in range(2):
                    row = pl.multiple_of(index * TILE + inner * 128, 128)
                    ones = keep_tile(dwords, tile * 8, row)
                    raw[slot, pl.ds(row, 128)] = raw[slot, pl.ds(row, 128)] * ones
                return carry

            lax.fori_loop(0, units // TILE, band, 0)
            tile_store(tile, slot).start()
            return carry

        lax.fori_loop(0, tiles, step, 0)
        tile_store(tiles - 1, (tiles - 1) % 2).wait()

    def square_sums(number, first):
        def step(block, carry):
            span = pl.ds(pl.multiple_of(block * TILE, TILE), TILE)
            total = jnp.zeros((1, TILE), F32)
            for chunk in GROUPS[number]:
                wide = hs[chunk, :, :, span].astype(F32)
                total = total + jnp.sum(jnp.sum(wide * wide, axis=0), axis=0, keepdims=True)
            if not first:
                total = total + hidden_norms[:, span]
            hidden_norms[:, span] = total
            return carry

        lax.fori_loop(0, blocks, step, 0)

    def input_sums():
        def step(tile, carry):
            span = pl.ds(pl.multiple_of(tile * TILE, TILE), TILE)

            def one(source, total):
                for piece in range(n_mp):
                    wide = xs[(source,) + piece_index(piece) + (every, span)].astype(F32)
                    total = total + jnp.sum(wide * wide, axis=0, keepdims=True)
                return total

            total = lax.fori_loop(0, n_dp, one, jnp.zeros((1, TILE), F32))
            input_norms[:, span] = jnp.sqrt(total)
            return carry

        lax.fori_loop(0, tiles, step, 0)

    def fold_copy(number, level, piece):
        span = pl.ds(pl.multiple_of(piece * PIECE, PIECE), PIECE)
        place = (every,) * (levels - level) + (1 - bits[level],) + tuple(bits[low] for low in reversed(range(level)))
        return remote(
            po[number].at[place + (every, span)],
            land[number][level].at[(every,) * (levels - level + 1) + (span,)],
            e_sem, (number, level, piece), p, across(level),
        )

    def project(number):
        group = GROUPS[number]
        tile_load(0, 0).start()

        def step(piece, carry):
            for half in range(PIECE // TILE):
                tile = piece * (PIECE // TILE) + half
                slot = half % 2
                tile_load(tile, slot).wait()

                @pl.when(tile + 1 < tiles)
                def _():
                    tile_load(tile + 1, 1 - slot).start()

                span = pl.ds(pl.multiple_of(tile * TILE, TILE), TILE)
                for place, chunk in enumerate(group):
                    left = hs[chunk].reshape(n_dp * small, units)
                    product = jnp.dot(left, raw[slot, pl.ds(0, units)], preferred_element_type=F32)
                    shape = (2,) * levels + (part, TILE)
                    po[number][(place,) + (every,) * (levels + 1) + (span,)] = product.astype(BF16).reshape(shape)
            fold_copy(number, 0, piece).start()
            return carry

        lax.fori_loop(0, pieces, step, 0)

    def fold(number, level):
        group = GROUPS[number]
        fixed = tuple(bits[low] for low in reversed(range(level + 1)))

        def step(piece, carry):
            span = pl.ds(pl.multiple_of(piece * PIECE, PIECE), PIECE)
            fold_copy(number, level, piece).wait()
            place = (every,) * (levels - level) + fixed + (every, span)
            other = land[number][level][(every,) * (levels - level + 1) + (span,)]
            total = (po[number][place].astype(F32) + other.astype(F32)).astype(BF16)
            if level + 1 < levels:
                po[number][place] = total
                fold_copy(number, level + 1, piece).start()
            else:
                for index, chunk in enumerate(group):
                    mixed[chunk * part : (chunk + 1) * part, span] = total[index]
            return carry

        lax.fori_loop(0, pieces, step, 0)

    def sums_sent(number):
        def step(block, carry):
            for shift in range(chips - 1):
                sum_copy(number, shift, block, chip_at(shift + 1)).wait_send()
            return carry

        lax.fori_loop(0, blocks, step, 0)

    own_load.wait()
    loads[0].wait()
    loads[1].wait()
    from_partner.wait_recv()
    if chips > 1:
        away(0, 0, first_prepare)
        away(1, 0)
        finish_spread()
        for shift in range(1, chips - 1):
            away(0, shift)
            away(1, shift)
    make_hidden(0)
    for shift in range(chips - 1):
        away(2, shift)
    input_sums()
    loads[2].wait()
    mask_down()
    make_hidden(1)
    gather_hidden(0)
    project(0)
    square_sums(0, True)
    make_hidden(2)
    fold(0, 0)
    fold(0, 1)
    gather_hidden(1)
    project(1)
    square_sums(1, False)
    for level in range(2, levels):
        fold(0, level)
    fold(1, 0)
    gather_hidden(2)
    project(2)
    square_sums(2, False)
    for level in range(1, levels):
        fold(1, level)
    for level in range(levels):
        fold(2, level)

    hidden_norms[...] = jnp.sqrt(hidden_norms[...])
    to_partner.wait_send()
    for number in range(len(GROUPS)):
        sums_sent(number)
        for chunk in GROUPS[number]:
            for shift in range(1, chips):
                hidden_copy(chunk, shift).wait_send()
            for shift in range(chips):
                partner_copy(chunk, shift, core).wait_send()


def on_device(
    n_dp, n_mp,
    tokens, norm_gain, gate_weight, gate_mask, up_weight, up_mask, down_weight, down_mask
):
    chips = n_dp // CORES
    levels = n_mp.bit_length() - 1
    rows, features = tokens.shape
    width, units = gate_weight.shape
    piece_rows = rows // n_mp
    blocks, tiles, pieces = units // TILE, width // TILE, width // PIECE
    small = rows // CHUNKS
    part = small * n_dp // n_mp
    away = chips - 1
    grid = (2,) * levels

    normed = normalise(tokens, norm_gain).reshape(grid + (piece_rows, features))
    counts = [len(group) for group in GROUPS]
    sums = [(away, blocks, small * count, 2 * TILE) for count in counts]
    dma = pltpu.SemaphoreType.DMA
    anywhere = pl.BlockSpec(memory_space=pl.ANY)
    vmem = pl.BlockSpec(memory_space=pltpu.VMEM)
    mixed, input_norms, hidden_norms, _ = pl.pallas_call(
        functools.partial(layer_kernel, n_dp, n_mp, levels),
        in_specs=[anywhere] * 7,
        out_specs=[vmem, vmem, vmem, anywhere],
        out_shape=[
            jax.ShapeDtypeStruct((CHUNKS * part, width), BF16),
            jax.ShapeDtypeStruct((1, width), F32),
            jax.ShapeDtypeStruct((1, units), F32),
            jax.ShapeDtypeStruct((tiles, units, TILE), BF16),
        ],
        scratch_shapes=[
            pltpu.VMEM((n_dp,) + grid + (piece_rows, width), BF16),
            pltpu.VMEM((blocks, width, 2 * TILE), BF16),
            pltpu.VMEM((2, max(2 * width, units), TILE), BF16),
            pltpu.VMEM((2, units // 32, width), jnp.int32),
            pltpu.VMEM((width // 32, units), jnp.int32),
            pltpu.VMEM((SLOTS, small * max(counts), 2 * TILE), BF16),
            pltpu.VMEM((SLOTS, small * max(counts), 2 * TILE), BF16),
            pltpu.VMEM((2, small * max(counts), 2 * TILE), F32),
            [pltpu.VMEM(shape, BF16) for shape in sums],
            [pltpu.VMEM(shape, BF16) for shape in sums],
            pltpu.VMEM((CHUNKS, n_dp, small, units), BF16),
            [pltpu.VMEM((count,) + grid + (part, width), BF16) for count in counts],
            [
                [pltpu.VMEM((count,) + grid[level + 1 :] + (part, width), BF16) for level in range(levels)]
                for count in counts
            ],
            dma((4,)),
            dma((2, 2)),
            dma((2, 2)),
            dma((2,)),
            dma((2, away, CORES, CORES)),
            dma((2, levels, away, CORES)),
            dma((2, SLOTS)),
            dma((2, len(GROUPS), away, blocks)),
            dma((2, CHUNKS, away)),
            dma((2, CHUNKS, chips)),
            dma((2, len(GROUPS), levels, pieces)),
        ],
        compiler_params=pltpu.CompilerParams(
            collective_id=0, has_side_effects=True, vmem_limit_bytes=67_043_328
        ),
        cost_estimate=pl.CostEstimate(
            flops=6 * rows * n_dp * width * units, bytes_accessed=10 * width * units, transcendentals=rows * units
        ),
    )(normed, gate_weight, up_weight, down_weight, gate_mask.T, up_mask.T, down_mask.T)
    return mixed, input_norms[0], hidden_norms[0]


def solution(mesh):
    n_dp, n_mp = mesh.shape["dp"], mesh.shape["mp"]

    def body(*args):
        return on_device(n_dp, n_mp, *args)

    return jax.shard_map(
        body,
        mesh=mesh,
        in_specs=(
            P("dp", None),
            P(),
            P("dp", "mp"),
            P("dp", "mp"),
            P("dp", "mp"),
            P("dp", "mp"),
            P("mp", "dp"),
            P("mp", "dp"),
        ),
        out_specs=(P("mp", "dp"), P("dp"), P("mp")),
        check_vma=False,
    )
```
